256 devices in a mesh: feat: 8 (over y, core), rows: 32 (over z, x).
Axes of the slice: x: 4, y: 4, z: 8, core: 2. Of those that a mesh axis runs over, the one named last changes fastest.
Arguments:
- bin_index: int32 [128, 262144], P('feat', 'rows'), may hold values from 0 to 255
- node_ids: int32 [262144], P('rows'), may hold values from 0 to 31
- gradients: int32 [262144], P('rows'), may hold values from -32 to 32
- hessians: int32 [262144], P('rows'), may hold values from 1 to 32
Outputs:
- split_gains: float32 [32, 128, 256], P('rows', 'feat')
- best_gains: float32 [32], P('rows')
The draws below stay inside these ranges and needn't reach their ends.
All inputs are finite; a program needn't handle non-finite values.
Results may differ from the reference program's by a relative error of at most 0.0003.
Values sent between devices are 32-bit elements; how exact they have to be, the bound alone decides.
A program may use at most 64 MiB of HBM per device.

```python
import math
import jax
import jax.numpy as jnp
import numpy as np

BINS = 256
ROWS = 262144
FEATURES = 128
NODES = 32


def with_ends(result, stream_key, least, largest):
    longest = result.shape.index(max(result.shape))
    spots = []
    for shift in (0, 1):
        where = [jax.random.randint(jax.random.fold_in(stream_key, axis), (), 0, length) for axis, length in enumerate(result.shape)]
        where[longest] = (where[longest] + shift) % result.shape[longest]
        spots.append(tuple(where))
    return result.at[spots[0]].set(least).at[spots[1]].set(largest)


def rank_bounds(count, lean):
    weights = [(1 << 20) // math.isqrt(grade ** lean) + 1 for grade in range(1, count + 1)]
    spread = 1 + sum(weights) // (1 << 30)
    return np.cumsum(np.array([max(1, weight // spread) for weight in weights]))


def ranked_ids(own_key, dims, number_of, lean):
    grid = rank_bounds(number_of, lean)
    ticket = jax.random.randint(jax.random.fold_in(own_key, 1), dims, 0, int(grid[number_of - 1]))
    rank = jnp.searchsorted(jnp.asarray(grid, jnp.int32), ticket, side="right")
    return jax.random.permutation(jax.random.fold_in(own_key, 2), number_of)[rank].astype(jnp.int32)


def setup_inputs(seed: int = 0) -> dict:
    seeds = jax.random.split(jax.random.key(seed), 5)
    bin_index = with_ends(jax.random.randint(seeds[0], (FEATURES, ROWS), 0, BINS), jax.random.fold_in(seeds[0], 1), 0, BINS - 1).astype(jnp.int32)
    node_ids = with_ends(ranked_ids(seeds[1], (ROWS,), NODES, 2), jax.random.fold_in(seeds[1], 3), 0, NODES - 1).astype(jnp.int32)
    gradients = with_ends(jax.random.randint(seeds[2], (ROWS,), -32, 33), jax.random.fold_in(seeds[2], 1), -32, 32).astype(jnp.int32)
    hessians = with_ends(jax.random.randint(seeds[3], (ROWS,), 1, 33), jax.random.fold_in(seeds[3], 1), 1, 32).astype(jnp.int32)
    return dict(bin_index=bin_index, node_ids=node_ids, gradients=gradients, hessians=hessians)


shrinkage = 1.0


def gains_of(grad_hist, hess_hist):
    left_grad = jnp.cumsum(grad_hist, axis=-1)
    left_hess = jnp.cumsum(hess_hist, axis=-1)
    total_grad = left_grad[..., -1:]
    total_hess = left_hess[..., -1:]
    right_grad = total_grad - left_grad
    right_hess = total_hess - left_hess
    return 0.5 * (left_grad * left_grad / (left_hess + shrinkage) + right_grad * right_grad / (right_hess + shrinkage) - total_grad * total_grad / (total_hess + shrinkage))


def reference(bin_index, node_ids, gradients, hessians):
    row_major = bin_index.T
    feature_ids = jnp.arange(FEATURES, dtype=jnp.int32)
    segment = ((node_ids[:, None] * FEATURES + feature_ids[None, :]) * BINS + row_major).astype(jnp.int32).reshape(-1)
    grad_rows = jnp.broadcast_to(gradients.astype(jnp.float32)[:, None], row_major.shape).reshape(-1)
    hess_rows = jnp.broadcast_to(hessians.astype(jnp.float32)[:, None], row_major.shape).reshape(-1)
    grad_hist = jax.ops.segment_sum(grad_rows, segment, NODES * FEATURES * BINS).reshape(NODES, FEATURES, BINS)
    hess_hist = jax.ops.segment_sum(hess_rows, segment, NODES * FEATURES * BINS).reshape(NODES, FEATURES, BINS)
    split_gains = gains_of(grad_hist, hess_hist)
    best_gains = jnp.max(split_gains, axis=(1, 2))
    return split_gains, best_gains
```

```python
import functools

import jax
import jax.numpy as jnp
from jax import lax
from jax.experimental import pallas as pl
from jax.experimental.pallas import tpu as pltpu
from jax.sharding import PartitionSpec as P

BINS = 256
HALF = 128
LANES = 128
BASE = 9
TOP = 8192
X = 4
Z = 8
FEAT = 8
GROUP = 4
BLOCK = 512
UNROLL = 16
shrinkage = 1.0
MESH = pl.DeviceIdType.MESH
f32 = jnp.float32
bf16 = jnp.bfloat16


def rows_of(row):
    return jnp.broadcast_to(row, (16, LANES)).astype(f32).astype(bf16)


def digit_rows(grad, hess):
    grad8 = jnp.broadcast_to(grad, (8, LANES))
    hess8 = jnp.broadcast_to(hess, (8, LANES))
    return jnp.concatenate([grad8, hess8], 0).astype(bf16)


def weights_of(node_ref, grad_ref, hess_ref, start, nodes_at):
    columns = []
    for tile in range(BLOCK // LANES):
        here = pl.ds(start + tile * LANES, LANES)
        node = rows_of(node_ref[0:1, here])
        grad = grad_ref[0:1, here].astype(f32)
        hess = hess_ref[0:1, here].astype(f32)
        grad_high = jnp.round(grad * (1.0 / BASE))
        hess_high = jnp.round(hess * (1.0 / BASE))
        low = digit_rows(grad - BASE * grad_high, hess - BASE * hess_high)
        high = digit_rows(grad_high, hess_high)
        none = jnp.zeros_like(low)
        masks = [node == nodes for nodes in nodes_at]
        column = [jnp.where(mask, low, none) for mask in masks]
        column += [jnp.where(mask, high, none) for mask in masks]
        columns.append(jnp.concatenate(column, 0))
    return jnp.concatenate(columns, 1)


def kernel(
    bins_ref,
    node_ref,
    grad_ref,
    hess_ref,
    out_ref,
    best_ref,
    weights,
    total,
    partial,
    x_in,
    z_out,
    z_in,
    best_out,
    best_in,
    x_send,
    x_recv,
    z_send,
    z_recv,
    b_send,
    b_recv,
):
    feature_count, row_count = bins_ref.shape
    groups = feature_count // GROUP
    feat = lax.axis_index("feat")
    rows = lax.axis_index("rows")
    my_z = rows // X
    my_x = rows % X

    x_peer = [my_z * X + (my_x + step) % X for step in range(X)]
    z_peer = [((my_z + step) % Z) * X + my_x for step in range(Z)]
    f_peer = [(feat + step) % FEAT for step in range(FEAT)]

    barrier = pltpu.get_barrier_semaphore()
    for step in range(1, X):
        pl.semaphore_signal(barrier, inc=1, device_id=(feat, x_peer[step]), device_id_type=MESH)
    for step in range(1, Z):
        pl.semaphore_signal(barrier, inc=1, device_id=(feat, z_peer[step]), device_id_type=MESH)
    for step in range(1, FEAT):
        pl.semaphore_signal(barrier, inc=1, device_id=(f_peer[step], rows), device_id_type=MESH)

    bin_at = lax.broadcasted_iota(jnp.int32, (HALF, LANES), 0).astype(f32).astype(bf16)
    nodes_at = [
        ((lax.broadcasted_iota(jnp.int32, (16, LANES), 0) % Z) * X + x).astype(f32).astype(bf16)
        for x in range(X)
    ]
    big = f32(1.5 * 2.0**36)

    def compute(group):
        def block(number, carry):
            start = pl.multiple_of(number * BLOCK, BLOCK)
            row_list = []
            for feature in range(GROUP):
                at = group * GROUP + feature
                columns = []
                for tile in range(BLOCK // LANES):
                    row = bins_ref[at : at + 1, pl.ds(start + tile * LANES, LANES)]
                    upper = row >= HALF
                    low = jnp.where(upper, row - HALF, row)
                    size = jnp.where(upper, TOP, 1)
                    low = jnp.concatenate([rows_of(low)] * (HALF // 16), 0)
                    size = jnp.concatenate([rows_of(size)] * (HALF // 16), 0)
                    columns.append(jnp.where(low <= bin_at, size, jnp.zeros_like(size)))
                row_list.append(jnp.concatenate(columns, 1))
            hot = jnp.concatenate(row_list, 0)
            if group == 0:
                weight = weights_of(node_ref, grad_ref, hess_ref, start, nodes_at)
                weights[:, pl.ds(start, BLOCK)] = weight
            else:
                weight = weights[:, pl.ds(start, BLOCK)]
            product = lax.dot_general(
                hot, weight, (((1,), (1,)), ((), ())), preferred_element_type=f32
            )
            upper_part = (product + big) - big
            total[0] += product - upper_part
            total[1] += upper_part
            return carry

        total[...] = jnp.zeros_like(total)
        lax.fori_loop(0, row_count // BLOCK, block, 0, unroll=UNROLL)
        for feature in range(GROUP):
            at = slice(feature * HALF, (feature + 1) * HALF)
            for half in range(2):
                turned = total[half, at, :].T
                joined = turned[: LANES // 2] + BASE * turned[LANES // 2 :]
                if half:
                    joined = joined * (1.0 / TOP)
                for x in range(X):
                    partial[group, x, feature, :, half * HALF : (half + 1) * HALF] = joined[
                        x * 16 : (x + 1) * 16
                    ]

    def x_copy(group, step):
        return pltpu.make_async_remote_copy(
            src_ref=partial.at[group, (my_x + step) % X],
            dst_ref=x_in.at[group, step - 1],
            send_sem=x_send.at[group, step - 1],
            recv_sem=x_recv.at[group, step - 1],
            device_id=(feat, x_peer[step]),
            device_id_type=MESH,
        )

    def z_copy(group, step):
        return pltpu.make_async_remote_copy(
            src_ref=z_out.at[group, (my_z + step) % Z],
            dst_ref=z_in.at[group, step - 1],
            send_sem=z_send.at[group, step - 1],
            recv_sem=z_recv.at[group, step - 1],
            device_id=(feat, z_peer[step]),
            device_id_type=MESH,
        )

    def best_copy(step):
        return pltpu.make_async_remote_copy(
            src_ref=best_out,
            dst_ref=best_in.at[step - 1],
            send_sem=b_send.at[step - 1],
            recv_sem=b_recv.at[step - 1],
            device_id=(f_peer[step], rows),
            device_id_type=MESH,
        )

    def start_x(group):
        for step in range(1, X):
            x_copy(group, step).start()

    def x_to_z(group):
        for step in range(1, X):
            x_copy(group, step).wait_recv()
        for feature in range(GROUP):
            summed = partial[group, my_x, feature]
            for step in range(1, X):
                summed = summed + x_in[group, step - 1, feature]
            for part in range(2):
                for z in range(Z):
                    z_out[group, z, part * GROUP + feature : part * GROUP + feature + 1, :] = summed[
                        part * Z + z : part * Z + z + 1
                    ]
        for step in range(1, Z):
            z_copy(group, step).start()

    def finish(group):
        for step in range(1, Z):
            z_copy(group, step).wait_recv()
        summed = z_out[group, my_z]
        for step in range(1, Z):
            summed = summed + z_in[group, step - 1]
        first = summed[:, :HALF]
        second = summed[:, HALF:] + first[:, HALF - 1 :]
        whole = second[:, HALF - 1 :]
        left = jnp.concatenate([first, second], 1)
        right = whole - left
        left_grad, left_hess = left[:GROUP], left[GROUP:]
        right_grad, right_hess = right[:GROUP], right[GROUP:]
        whole_grad, whole_hess = whole[:GROUP], whole[GROUP:]
        gains = 0.5 * (
            left_grad * left_grad / (left_hess + shrinkage)
            + right_grad * right_grad / (right_hess + shrinkage)
            - whole_grad * whole_grad / (whole_hess + shrinkage)
        )
        out_ref[0, group * GROUP : (group + 1) * GROUP, :] = gains

    for group in range(groups):
        compute(group)
        if group == 0:
            pl.semaphore_wait(barrier, X - 1 + Z - 1 + FEAT - 1)
        start_x(group)
        if group >= 1:
            x_to_z(group - 1)
        if group >= 2:
            finish(group - 2)
    x_to_z(groups - 1)
    finish(groups - 2)
    finish(groups - 1)
    gains = out_ref[0]
    top = jnp.max(jnp.max(gains, axis=1, keepdims=True), axis=0, keepdims=True)
    best_out[...] = jnp.broadcast_to(top, best_out.shape)
    for step in range(1, FEAT):
        best_copy(step).start()
    best = best_out[...]
    for step in range(1, FEAT):
        best_copy(step).wait_recv()
        best = jnp.maximum(best, best_in[step - 1])
    best_ref[...] = best
    for group in range(groups):
        for step in range(1, X):
            x_copy(group, step).wait_send()
        for step in range(1, Z):
            z_copy(group, step).wait_send()
    for step in range(1, FEAT):
        best_copy(step).wait_send()


def per_device(bin_index, node_ids, gradients, hessians):
    feature_count, row_count = bin_index.shape
    groups = feature_count // GROUP
    vmem = pl.BlockSpec(memory_space=pltpu.VMEM)
    dma = pltpu.SemaphoreType.DMA
    gains, best = pl.pallas_call(
        kernel,
        out_shape=(
            jax.ShapeDtypeStruct((1, feature_count, BINS), f32),
            jax.ShapeDtypeStruct((8, LANES), f32),
        ),
        in_specs=[vmem] * 4,
        out_specs=(vmem, vmem),
        scratch_shapes=[
            pltpu.VMEM((LANES, row_count), bf16),
            pltpu.VMEM((2, GROUP * HALF, LANES), f32),
            pltpu.VMEM((groups, X, GROUP, 2 * Z, BINS), f32),
            pltpu.VMEM((groups, X - 1, GROUP, 2 * Z, BINS), f32),
            pltpu.VMEM((groups, Z, 2 * GROUP, BINS), f32),
            pltpu.VMEM((groups, Z - 1, 2 * GROUP, BINS), f32),
            pltpu.VMEM((8, LANES), f32),
            pltpu.VMEM((FEAT - 1, 8, LANES), f32),
            dma((groups, X - 1)),
            dma((groups, X - 1)),
            dma((groups, Z - 1)),
            dma((groups, Z - 1)),
            dma((FEAT - 1,)),
            dma((FEAT - 1,)),
        ],
        compiler_params=pltpu.CompilerParams(
            collective_id=0, has_side_effects=True, vmem_limit_bytes=48 * 2**20
        ),
    )(
        bin_index,
        node_ids.reshape(1, row_count),
        gradients.reshape(1, row_count),
        hessians.reshape(1, row_count),
    )
    return gains, best[0, :1]


def solution(mesh):
    in_specs = (P("feat", "rows"), P("rows"), P("rows"), P("rows"))
    out_specs = (P("rows", "feat", None), P("rows"))
    return jax.shard_map(
        per_device, mesh=mesh, in_specs=in_specs, out_specs=out_specs, check_vma=False
    )
```

```python
import functools

import jax
import jax.numpy as jnp
from jax import lax
from jax.experimental import pallas as pl
from jax.experimental.pallas import tpu as pltpu
from jax.sharding import PartitionSpec as P

BINS = 256
HALF = 128
LANES = 128
BASE = 9
TOP = 8192
X = 4
Z = 8
FEAT = 8
GROUPS = (4, 4, 4, 2, 2)
RELAYED = 4
LAGS = (4, 8, 14)
BLOCK = 512
UNROLL = 16
shrinkage = 1.0
MESH = pl.DeviceIdType.MESH
f32 = jnp.float32
bf16 = jnp.bfloat16


def rows_of(row):
    return jnp.broadcast_to(row, (16, LANES)).astype(f32).astype(bf16)


def digit_rows(grad, hess):
    grad8 = jnp.broadcast_to(grad, (8, LANES))
    hess8 = jnp.broadcast_to(hess, (8, LANES))
    return jnp.concatenate([grad8, hess8], 0).astype(bf16)


def weights_of(node_ref, grad_ref, hess_ref, start, nodes_at):
    columns = []
    for tile in range(BLOCK // LANES):
        here = pl.ds(start + tile * LANES, LANES)
        node = rows_of(node_ref[0:1, here])
        grad = grad_ref[0:1, here].astype(f32)
        hess = hess_ref[0:1, here].astype(f32)
        grad_high = jnp.round(grad * (1.0 / BASE))
        hess_high = jnp.round(hess * (1.0 / BASE))
        low = digit_rows(grad - BASE * grad_high, hess - BASE * hess_high)
        high = digit_rows(grad_high, hess_high)
        none = jnp.zeros_like(low)
        masks = [node == nodes for nodes in nodes_at]
        column = [jnp.where(mask, low, none) for mask in masks]
        column += [jnp.where(mask, high, none) for mask in masks]
        columns.append(jnp.concatenate(column, 0))
    return jnp.concatenate(columns, 1)


def kernel(*refs):
    groups = len(GROUPS)
    take = iter(refs)
    some = lambda count: [next(take) for unused in range(count)]
    bins_hbm, node_hbm, grad_hbm, hess_hbm, out_ref, best_ref = some(6)
    bins_ref, node_ref, grad_ref, hess_ref, weights, total = some(6)
    partial, x_in, z_out, z_in = some(groups), some(groups), some(groups), some(groups)
    relay_in, relay_out = some(RELAYED), some(RELAYED)
    best_out, best_in, load_sem = some(3)
    x_send, x_recv, r_send, r_recv, z_send, z_recv, b_send, b_recv = some(8)

    feature_count, row_count = bins_ref.shape
    feat = lax.axis_index("feat")
    rows = lax.axis_index("rows")
    my_z = rows // X
    my_x = rows % X

    loads = [
        pltpu.make_async_copy(source, target, load_sem.at[number])
        for number, (source, target) in enumerate(
            [
                (node_hbm, node_ref),
                (grad_hbm, grad_ref),
                (hess_hbm, hess_ref),
                (bins_hbm.at[0:8], bins_ref.at[0:8]),
                (bins_hbm.at[8:16], bins_ref.at[8:16]),
            ]
        )
    ]
    for load in loads:
        load.start()

    def device_at(z, x):
        return ((my_z + z) % Z) * X + (my_x + x) % X

    barrier = pltpu.get_barrier_semaphore()
    for step in range(1, X):
        pl.semaphore_signal(
            barrier, inc=1, device_id=(feat, device_at(0, step)), device_id_type=MESH
        )
    for step in range(1, Z):
        pl.semaphore_signal(
            barrier, inc=1, device_id=(feat, device_at(step, 0)), device_id_type=MESH
        )
    for step in range(1, FEAT):
        pl.semaphore_signal(
            barrier, inc=1, device_id=((feat + step) % FEAT, rows), device_id_type=MESH
        )

    bin_at = lax.broadcasted_iota(jnp.int32, (HALF, LANES), 0).astype(f32).astype(bf16)
    nodes_at = [
        ((lax.broadcasted_iota(jnp.int32, (16, LANES), 0) % Z) * X + x).astype(f32).astype(bf16)
        for x in range(X)
    ]
    big = f32(1.5 * 2.0**36)

    def compute(group):
        size_here = GROUPS[group]
        base = sum(GROUPS[:group])
        totals = slice(0, size_here * HALF)

        def block(number, carry):
            start = pl.multiple_of(number * BLOCK, BLOCK)
            row_list = []
            for feature in range(size_here):
                at = base + feature
                columns = []
                for tile in range(BLOCK // LANES):
                    row = bins_ref[at : at + 1, pl.ds(start + tile * LANES, LANES)]
                    upper = row >= HALF
                    low = jnp.where(upper, row - HALF, row)
                    size = jnp.where(upper, TOP, 1)
                    low = jnp.concatenate([rows_of(low)] * (HALF // 16), 0)
                    size = jnp.concatenate([rows_of(size)] * (HALF // 16), 0)
                    columns.append(jnp.where(low <= bin_at, size, jnp.zeros_like(size)))
                row_list.append(jnp.concatenate(columns, 1))
            hot = jnp.concatenate(row_list, 0)
            if group == 0:
                weight = weights_of(node_ref, grad_ref, hess_ref, start, nodes_at)
                weights[:, pl.ds(start, BLOCK)] = weight
            else:
                weight = weights[:, pl.ds(start, BLOCK)]
            product = lax.dot_general(
                hot, weight, (((1,), (1,)), ((), ())), preferred_element_type=f32
            )
            upper_part = (product + big) - big
            total[0, totals, :] += product - upper_part
            total[1, totals, :] += upper_part
            return carry

        total[:, totals, :] = jnp.zeros((2, size_here * HALF, LANES), f32)
        lax.fori_loop(0, row_count // BLOCK, block, 0, unroll=UNROLL)
        count = 4 * size_here
        for feature in range(size_here):
            at = slice(feature * HALF, (feature + 1) * HALF)
            for half in range(2):
                turned = total[half, at, :].T
                joined = turned[: LANES // 2] + BASE * turned[LANES // 2 :]
                if half:
                    joined = joined * (1.0 / TOP)
                for x in range(X):
                    for part in range(2):
                        line = (half * 2 + part) * size_here + feature
                        from_row = x * 2 * Z + part * Z
                        partial[group][pl.ds(x * Z * count + line, Z, stride=count), :] = joined[
                            from_row : from_row + Z
                        ]

    def lines_for(group, step):
        lines = 4 * GROUPS[group] * Z
        return pl.multiple_of(((my_x + step) % X) * lines, lines), lines

    def send(source, target, send_sem, recv_sem, device):
        return pltpu.make_async_remote_copy(
            src_ref=source,
            dst_ref=target,
            send_sem=send_sem,
            recv_sem=recv_sem,
            device_id=(feat, device),
            device_id_type=MESH,
        )

    def x_copy(group, step):
        start, lines = lines_for(group, step)
        return send(
            partial[group].at[pl.ds(start, lines)],
            x_in[group].at[step - 1],
            x_send.at[group, step - 1],
            x_recv.at[group, step - 1],
            device_at(0, step),
        )

    def far_copy(group, way):
        start, lines = lines_for(group, 2)
        half = lines // 2
        return send(
            partial[group].at[pl.ds(start + way * half, half)],
            relay_in[group].at[way],
            r_send.at[group, way],
            r_recv.at[group, way],
            device_at(0, 1 - 2 * way),
        )

    def plain_copy(group, way):
        start, lines = lines_for(group, 1 - 2 * way)
        half = lines // 2
        return send(
            partial[group].at[pl.ds(start + (1 - way) * half, half)],
            x_in[group].at[way, pl.ds((1 - way) * half, half)],
            x_send.at[group, way],
            x_recv.at[group, way],
            device_at(0, 1 - 2 * way),
        )

    def added_copy(group, way):
        half = 4 * GROUPS[group] * Z // 2
        return send(
            relay_out[group].at[way],
            x_in[group].at[way, pl.ds(way * half, half)],
            r_send.at[group, 2 + way],
            r_recv.at[group, 2 + way],
            device_at(0, 1 - 2 * way),
        )

    def z_copy(group, step):
        lines = 4 * GROUPS[group]
        source = pl.multiple_of(((my_z + step) % Z) * lines, lines)
        return pltpu.make_async_remote_copy(
            src_ref=z_out[group].at[pl.ds(source, lines)],
            dst_ref=z_in[group].at[step - 1],
            send_sem=z_send.at[group, step - 1],
            recv_sem=z_recv.at[group, step - 1],
            device_id=(feat, device_at(step, 0)),
            device_id_type=MESH,
        )

    def best_copy(step):
        return pltpu.make_async_remote_copy(
            src_ref=best_out,
            dst_ref=best_in.at[step - 1],
            send_sem=b_send.at[step - 1],
            recv_sem=b_recv.at[step - 1],
            device_id=((feat + step) % FEAT, rows),
            device_id_type=MESH,
        )

    def start_x(group):
        if group < RELAYED:
            for way in range(2):
                far_copy(group, way).start()
            for way in range(2):
                plain_copy(group, way).start()
        else:
            for step in (2, 1, 3):
                x_copy(group, step).start()

    def relay(group):
        for way in range(2):
            far_copy(group, way).wait_recv()
            start, lines = lines_for(group, 1 - 2 * way)
            half = lines // 2
            mine = partial[group][pl.ds(start + way * half, half), :]
            relay_out[group][way] = relay_in[group][way] + mine
            added_copy(group, way).start()

    def x_to_z(group):
        start, lines = lines_for(group, 0)
        summed = partial[group][pl.ds(start, lines), :]
        if group < RELAYED:
            for way in range(2):
                plain_copy(group, way).wait_recv()
                added_copy(group, way).wait_recv()
                summed = summed + x_in[group][way]
        else:
            for step in range(1, X):
                x_copy(group, step).wait_recv()
                summed = summed + x_in[group][step - 1]
        z_out[group][...] = summed
        for step in (4, 3, 5, 2, 6, 1, 7):
            z_copy(group, step).start()

    def gains_at(group, summed):
        size = GROUPS[group]
        base = sum(GROUPS[:group])
        first = summed[: 2 * size]
        second = summed[2 * size :] + first[:, HALF - 1 :]
        whole = second[:, HALF - 1 :]
        whole_grad, whole_hess = whole[:size], whole[size:]
        unsplit = whole_grad * whole_grad / (whole_hess + shrinkage)
        for half, left in enumerate((first, second)):
            right = whole - left
            left_grad, left_hess = left[:size], left[size:]
            right_grad, right_hess = right[:size], right[size:]
            out_ref[0, base : base + size, half * HALF : (half + 1) * HALF] = 0.5 * (
                left_grad * left_grad / (left_hess + shrinkage)
                + right_grad * right_grad / (right_hess + shrinkage)
                - unsplit
            )

    def finish(group):
        for step in range(1, Z):
            z_copy(group, step).wait_recv()
        lines = 4 * GROUPS[group]
        summed = z_out[group][pl.ds(pl.multiple_of(my_z * lines, lines), lines), :]
        for step in range(1, Z):
            summed = summed + z_in[group][step - 1]
        gains_at(group, summed)

    for number in range(4):
        loads[number].wait()
    events = []
    done = 0
    for group in range(groups):
        done += GROUPS[group]
        relayed = group < RELAYED
        if relayed:
            events.append((done + LAGS[0], 0, group, relay))
        events.append((done + LAGS[relayed], 1, group, x_to_z))
        events.append((done + LAGS[relayed] + LAGS[2] - LAGS[1], 2, group, finish))
    events.sort(key=lambda event: event[:3])
    done = 0
    for group in range(groups):
        compute(group)
        done += GROUPS[group]
        if group == 0:
            loads[4].wait()
            pl.semaphore_wait(barrier, X - 1 + Z - 1 + FEAT - 1)
        start_x(group)
        while events and (events[0][0] <= done or group == groups - 1):
            unused_time, unused_stage, which, action = events.pop(0)
            action(which)
    gains = out_ref[0]
    top = jnp.max(jnp.max(gains, axis=1, keepdims=True), axis=0, keepdims=True)
    best_out[...] = jnp.broadcast_to(top, best_out.shape)
    for step in range(1, FEAT):
        best_copy(step).start()
    for group in range(groups):
        if group < RELAYED:
            for way in range(2):
                far_copy(group, way).wait_send()
                plain_copy(group, way).wait_send()
                added_copy(group, way).wait_send()
        else:
            for step in range(1, X):
                x_copy(group, step).wait_send()
        for step in range(1, Z):
            z_copy(group, step).wait_send()
    best = best_out[...]
    for step in range(1, FEAT):
        best_copy(step).wait_recv()
        best = jnp.maximum(best, best_in[step - 1])
    best_ref[...] = best
    for step in range(1, FEAT):
        best_copy(step).wait_send()


def per_device(bin_index, node_ids, gradients, hessians):
    feature_count, row_count = bin_index.shape
    groups = len(GROUPS)
    vmem = pl.BlockSpec(memory_space=pltpu.VMEM)
    hbm = pl.BlockSpec(memory_space=pltpu.HBM)
    dma = pltpu.SemaphoreType.DMA
    table = lambda *shape: pltpu.VMEM((*shape, LANES), f32)
    gains, best = pl.pallas_call(
        kernel,
        out_shape=(
            jax.ShapeDtypeStruct((1, feature_count, BINS), f32),
            jax.ShapeDtypeStruct((8, LANES), f32),
        ),
        in_specs=[hbm] * 4,
        out_specs=(vmem, vmem),
        scratch_shapes=[
            pltpu.VMEM((feature_count, row_count), jnp.int32),
            *[pltpu.VMEM((1, row_count), jnp.int32)] * 3,
            pltpu.VMEM((LANES, row_count), bf16),
            table(2, max(GROUPS) * HALF),
            *[table(X * Z * 4 * size) for size in GROUPS],
            *[table(X - 1, Z * 4 * size) for size in GROUPS],
            *[table(Z * 4 * size) for size in GROUPS],
            *[table(Z - 1, 4 * size) for size in GROUPS],
            *[table(2, Z * 2 * size) for size in GROUPS[:RELAYED]] * 2,
            table(8),
            table(FEAT - 1, 8),
            dma((5,)),
            dma((groups, X - 1)),
            dma((groups, X - 1)),
            dma((groups, 4)),
            dma((groups, 4)),
            dma((groups, Z - 1)),
            dma((groups, Z - 1)),
            dma((FEAT - 1,)),
            dma((FEAT - 1,)),
        ],
        compiler_params=pltpu.CompilerParams(
            collective_id=0, has_side_effects=True, vmem_limit_bytes=55200 * 1024
        ),
    )(
        bin_index,
        node_ids.reshape(1, row_count),
        gradients.reshape(1, row_count),
        hessians.reshape(1, row_count),
    )
    return gains, best[0, :1]


def solution(mesh):
    in_specs = (P("feat", "rows"), P("rows"), P("rows"), P("rows"))
    out_specs = (P("rows", "feat", None), P("rows"))
    return jax.shard_map(
        per_device, mesh=mesh, in_specs=in_specs, out_specs=out_specs, check_vma=False
    )
```

```python
import functools

import jax
import jax.numpy as jnp
from jax import lax
from jax.experimental import pallas as pl
from jax.experimental.pallas import tpu as pltpu
from jax.sharding import PartitionSpec as P

BINS = 256
HALF = 128
LANES = 128
BASE = 9
TOP = 8192
X = 4
Z = 8
FEAT = 8
GROUPS = (5, 5, 4, 2)
MODES = "rzdd"
LAGS = (4, 9, 20)
BLOCK = 512
UNROLL = 16
shrinkage = 1.0
MESH = pl.DeviceIdType.MESH
f32 = jnp.float32
bf16 = jnp.bfloat16


def rows_of(row):
    return jnp.broadcast_to(row, (16, LANES)).astype(f32).astype(bf16)


def digit_rows(grad, hess):
    grad8 = jnp.broadcast_to(grad, (8, LANES))
    hess8 = jnp.broadcast_to(hess, (8, LANES))
    return jnp.concatenate([grad8, hess8], 0).astype(bf16)


def weights_of(node_ref, grad_ref, hess_ref, start, nodes_at):
    columns = []
    for tile in range(BLOCK // LANES):
        here = pl.ds(start + tile * LANES, LANES)
        node = rows_of(node_ref[0:1, here])
        grad = grad_ref[0:1, here].astype(f32)
        hess = hess_ref[0:1, here].astype(f32)
        grad_high = jnp.round(grad * (1.0 / BASE))
        hess_high = jnp.round(hess * (1.0 / BASE))
        low = digit_rows(grad - BASE * grad_high, hess - BASE * hess_high)
        high = digit_rows(grad_high, hess_high)
        none = jnp.zeros_like(low)
        masks = [node == nodes for nodes in nodes_at]
        column = [jnp.where(mask, low, none) for mask in masks]
        column += [jnp.where(mask, high, none) for mask in masks]
        columns.append(jnp.concatenate(column, 0))
    return jnp.concatenate(columns, 1)


def kernel(*refs):
    groups = len(GROUPS)
    take = iter(refs)
    some = lambda count: [next(take) for unused in range(count)]
    bins_hbm, node_hbm, grad_hbm, hess_hbm, out_ref, best_ref = some(6)
    bins_ref, node_ref, grad_ref, hess_ref, weights, total = some(6)
    partial, x_in, z_out, z_in = some(groups), some(groups), some(groups), some(groups)
    relay_in, relay_out = some(groups), some(groups)
    best_out, best_in, load_sem = some(3)
    x_send, x_recv, r_send, r_recv, z_send, z_recv, b_send, b_recv = some(8)

    feature_count, row_count = bins_ref.shape
    feat = lax.axis_index("feat")
    rows = lax.axis_index("rows")
    my_z = rows // X
    my_x = rows % X

    loads = [
        pltpu.make_async_copy(source, target, load_sem.at[number])
        for number, (source, target) in enumerate(
            [
                (node_hbm, node_ref),
                (grad_hbm, grad_ref),
                (hess_hbm, hess_ref),
                (bins_hbm.at[0:8], bins_ref.at[0:8]),
                (bins_hbm.at[8:16], bins_ref.at[8:16]),
            ]
        )
    ]
    for load in loads:
        load.start()

    def device_at(z, x):
        return ((my_z + z) % Z) * X + (my_x + x) % X

    barrier = pltpu.get_barrier_semaphore()
    for step in range(1, X):
        pl.semaphore_signal(
            barrier, inc=1, device_id=(feat, device_at(0, step)), device_id_type=MESH
        )
    for step in range(1, Z):
        pl.semaphore_signal(
            barrier, inc=1, device_id=(feat, device_at(step, 0)), device_id_type=MESH
        )
    for step in range(1, FEAT):
        pl.semaphore_signal(
            barrier, inc=1, device_id=((feat + step) % FEAT, rows), device_id_type=MESH
        )

    bin_at = lax.broadcasted_iota(jnp.int32, (HALF, LANES), 0).astype(f32).astype(bf16)
    nodes_at = [
        ((lax.broadcasted_iota(jnp.int32, (16, LANES), 0) % Z) * X + x).astype(f32).astype(bf16)
        for x in range(X)
    ]
    big = f32(1.5 * 2.0**36)

    def compute(group):
        size_here = GROUPS[group]
        base = sum(GROUPS[:group])
        totals = slice(0, size_here * HALF)

        def block(number, carry):
            start = pl.multiple_of(number * BLOCK, BLOCK)
            row_list = []
            for feature in range(size_here):
                at = base + feature
                columns = []
                for tile in range(BLOCK // LANES):
                    row = bins_ref[at : at + 1, pl.ds(start + tile * LANES, LANES)]
                    upper = row >= HALF
                    low = jnp.where(upper, row - HALF, row)
                    size = jnp.where(upper, TOP, 1)
                    low = jnp.concatenate([rows_of(low)] * (HALF // 16), 0)
                    size = jnp.concatenate([rows_of(size)] * (HALF // 16), 0)
                    columns.append(jnp.where(low <= bin_at, size, jnp.zeros_like(size)))
                row_list.append(jnp.concatenate(columns, 1))
            hot = jnp.concatenate(row_list, 0)
            if group == 0:
                weight = weights_of(node_ref, grad_ref, hess_ref, start, nodes_at)
                weights[:, pl.ds(start, BLOCK)] = weight
            else:
                weight = weights[:, pl.ds(start, BLOCK)]
            product = lax.dot_general(
                hot, weight, (((1,), (1,)), ((), ())), preferred_element_type=f32
            )
            upper_part = (product + big) - big
            total[0, totals, :] += product - upper_part
            total[1, totals, :] += upper_part
            return carry

        total[:, totals, :] = jnp.zeros((2, size_here * HALF, LANES), f32)
        lax.fori_loop(0, row_count // BLOCK, block, 0, unroll=UNROLL)
        count = 4 * size_here
        for feature in range(size_here):
            at = slice(feature * HALF, (feature + 1) * HALF)
            for half in range(2):
                turned = total[half, at, :].T
                joined = turned[: LANES // 2] + BASE * turned[LANES // 2 :]
                if half:
                    joined = joined * (1.0 / TOP)
                for x in range(X):
                    for part in range(2):
                        line = (half * 2 + part) * size_here + feature
                        from_row = x * 2 * Z + part * Z
                        if MODES[group] == "z":
                            lines = pl.ds(x * count + line, Z, stride=X * count)
                        else:
                            lines = pl.ds(x * Z * count + line, Z, stride=count)
                        partial[group][lines, :] = joined[from_row : from_row + Z]

    def lines_for(group, step):
        lines = 4 * GROUPS[group] * Z
        return pl.multiple_of(((my_x + step) % X) * lines, lines), lines

    def send(source, target, send_sem, recv_sem, device):
        return pltpu.make_async_remote_copy(
            src_ref=source,
            dst_ref=target,
            send_sem=send_sem,
            recv_sem=recv_sem,
            device_id=(feat, device),
            device_id_type=MESH,
        )

    def x_copy(group, step):
        start, lines = lines_for(group, step)
        return send(
            partial[group].at[pl.ds(start, lines)],
            x_in[group].at[step - 1],
            x_send.at[group, step - 1],
            x_recv.at[group, step - 1],
            device_at(0, step),
        )

    def far_copy(group, way):
        start, lines = lines_for(group, 2)
        half = lines // 2
        return send(
            partial[group].at[pl.ds(start + way * half, half)],
            relay_in[group].at[way],
            r_send.at[group, way],
            r_recv.at[group, way],
            device_at(0, 1 - 2 * way),
        )

    def plain_copy(group, way):
        start, lines = lines_for(group, 1 - 2 * way)
        half = lines // 2
        return send(
            partial[group].at[pl.ds(start + (1 - way) * half, half)],
            x_in[group].at[way, pl.ds((1 - way) * half, half)],
            x_send.at[group, way],
            x_recv.at[group, way],
            device_at(0, 1 - 2 * way),
        )

    def added_copy(group, way):
        half = 4 * GROUPS[group] * Z // 2
        return send(
            relay_out[group].at[way],
            x_in[group].at[way, pl.ds(way * half, half)],
            r_send.at[group, 2 + way],
            r_recv.at[group, 2 + way],
            device_at(0, 1 - 2 * way),
        )

    def z_copy(group, step):
        lines = 4 * GROUPS[group]
        source = pl.multiple_of(((my_z + step) % Z) * lines, lines)
        return pltpu.make_async_remote_copy(
            src_ref=z_out[group].at[pl.ds(source, lines)],
            dst_ref=z_in[group].at[step - 1],
            send_sem=z_send.at[group, step - 1],
            recv_sem=z_recv.at[group, step - 1],
            device_id=(feat, device_at(step, 0)),
            device_id_type=MESH,
        )

    def z_first_copy(group, step):
        lines = 4 * GROUPS[group] * X
        start = pl.multiple_of(((my_z + step) % Z) * lines, lines)
        return send(
            partial[group].at[pl.ds(start, lines)],
            x_in[group].at[step - 1],
            x_send.at[group, step - 1],
            x_recv.at[group, step - 1],
            device_at(step, 0),
        )

    def x_last_copy(group, step):
        lines = 4 * GROUPS[group]
        start = pl.multiple_of(((my_x + step) % X) * lines, lines)
        return send(
            z_out[group].at[pl.ds(start, lines)],
            z_in[group].at[step - 1],
            z_send.at[group, step - 1],
            z_recv.at[group, step - 1],
            device_at(0, step),
        )

    def best_copy(step):
        return pltpu.make_async_remote_copy(
            src_ref=best_out,
            dst_ref=best_in.at[step - 1],
            send_sem=b_send.at[step - 1],
            recv_sem=b_recv.at[step - 1],
            device_id=((feat + step) % FEAT, rows),
            device_id_type=MESH,
        )

    def start_x(group):
        if MODES[group] == "r":
            for way in range(2):
                far_copy(group, way).start()
            for way in range(2):
                plain_copy(group, way).start()
        elif MODES[group] == "z":
            for step in (4, 3, 5, 2, 6, 1, 7):
                z_first_copy(group, step).start()
        else:
            for step in (2, 1, 3):
                x_copy(group, step).start()

    def relay(group):
        for way in range(2):
            far_copy(group, way).wait_recv()
            start, lines = lines_for(group, 1 - 2 * way)
            half = lines // 2
            mine = partial[group][pl.ds(start + way * half, half), :]
            relay_out[group][way] = relay_in[group][way] + mine
            added_copy(group, way).start()

    def z_to_x(group):
        lines = 4 * GROUPS[group] * X
        summed = partial[group][pl.ds(pl.multiple_of(my_z * lines, lines), lines), :]
        for step in range(1, Z):
            z_first_copy(group, step).wait_recv()
            summed = summed + x_in[group][step - 1]
        z_out[group][...] = summed
        for step in (2, 1, 3):
            x_last_copy(group, step).start()

    def x_to_z(group):
        if MODES[group] == "z":
            return z_to_x(group)
        start, lines = lines_for(group, 0)
        summed = partial[group][pl.ds(start, lines), :]
        if MODES[group] == "r":
            for way in range(2):
                plain_copy(group, way).wait_recv()
                added_copy(group, way).wait_recv()
                summed = summed + x_in[group][way]
        else:
            for step in range(1, X):
                x_copy(group, step).wait_recv()
                summed = summed + x_in[group][step - 1]
        z_out[group][...] = summed
        for step in (4, 3, 5, 2, 6, 1, 7):
            z_copy(group, step).start()

    def gains_at(group, summed):
        size = GROUPS[group]
        base = sum(GROUPS[:group])
        first = summed[: 2 * size]
        second = summed[2 * size :] + first[:, HALF - 1 :]
        whole = second[:, HALF - 1 :]
        whole_grad, whole_hess = whole[:size], whole[size:]
        unsplit = whole_grad * whole_grad / (whole_hess + shrinkage)
        for half, left in enumerate((first, second)):
            right = whole - left
            left_grad, left_hess = left[:size], left[size:]
            right_grad, right_hess = right[:size], right[size:]
            out_ref[0, base : base + size, half * HALF : (half + 1) * HALF] = 0.5 * (
                left_grad * left_grad / (left_hess + shrinkage)
                + right_grad * right_grad / (right_hess + shrinkage)
                - unsplit
            )

    def finish(group):
        if MODES[group] == "z":
            lines = 4 * GROUPS[group]
            summed = z_out[group][pl.ds(pl.multiple_of(my_x * lines, lines), lines), :]
            for step in range(1, X):
                x_last_copy(group, step).wait_recv()
                summed = summed + z_in[group][step - 1]
            return gains_at(group, summed)
        for step in range(1, Z):
            z_copy(group, step).wait_recv()
        lines = 4 * GROUPS[group]
        summed = z_out[group][pl.ds(pl.multiple_of(my_z * lines, lines), lines), :]
        for step in range(1, Z):
            summed = summed + z_in[group][step - 1]
        gains_at(group, summed)

    for number in range(4):
        loads[number].wait()
    events = []
    done = 0
    for group in range(groups):
        done += GROUPS[group]
        relayed = MODES[group] != "d"
        if MODES[group] == "r":
            events.append((done + LAGS[0], 0, group, relay))
        events.append((done + LAGS[relayed], 1, group, x_to_z))
        events.append((done + LAGS[relayed] + LAGS[2] - LAGS[1], 2, group, finish))
    events.sort(key=lambda event: event[:3])
    done = 0
    for group in range(groups):
        compute(group)
        done += GROUPS[group]
        if group == 0:
            loads[4].wait()
            pl.semaphore_wait(barrier, X - 1 + Z - 1 + FEAT - 1)
        start_x(group)
        while events and (events[0][0] <= done or group == groups - 1):
            unused_time, unused_stage, which, action = events.pop(0)
            action(which)
    gains = out_ref[0]
    top = jnp.max(jnp.max(gains, axis=1, keepdims=True), axis=0, keepdims=True)
    best_out[...] = jnp.broadcast_to(top, best_out.shape)
    for step in range(1, FEAT):
        best_copy(step).start()
    for group in range(groups):
        if MODES[group] == "r":
            for way in range(2):
                far_copy(group, way).wait_send()
                plain_copy(group, way).wait_send()
                added_copy(group, way).wait_send()
        elif MODES[group] == "d":
            for step in range(1, X):
                x_copy(group, step).wait_send()
        if MODES[group] == "z":
            for step in range(1, Z):
                z_first_copy(group, step).wait_send()
            for step in range(1, X):
                x_last_copy(group, step).wait_send()
        else:
            for step in range(1, Z):
                z_copy(group, step).wait_send()
    best = best_out[...]
    for step in range(1, FEAT):
        best_copy(step).wait_recv()
        best = jnp.maximum(best, best_in[step - 1])
    best_ref[...] = best
    for step in range(1, FEAT):
        best_copy(step).wait_send()


def per_device(bin_index, node_ids, gradients, hessians):
    feature_count, row_count = bin_index.shape
    groups = len(GROUPS)
    vmem = pl.BlockSpec(memory_space=pltpu.VMEM)
    hbm = pl.BlockSpec(memory_space=pltpu.HBM)
    dma = pltpu.SemaphoreType.DMA
    stages = [(size, *((Z, X) if mode == "z" else (X, Z))) for size, mode in zip(GROUPS, MODES)]
    table = lambda *shape: pltpu.VMEM((*shape, LANES), f32)
    gains, best = pl.pallas_call(
        kernel,
        out_shape=(
            jax.ShapeDtypeStruct((1, feature_count, BINS), f32),
            jax.ShapeDtypeStruct((8, LANES), f32),
        ),
        in_specs=[hbm] * 4,
        out_specs=(vmem, vmem),
        scratch_shapes=[
            pltpu.VMEM((feature_count, row_count), jnp.int32),
            *[pltpu.VMEM((1, row_count), jnp.int32)] * 3,
            pltpu.VMEM((LANES, row_count), bf16),
            table(2, max(GROUPS) * HALF),
            *[table(X * Z * 4 * size) for size in GROUPS],
            *[table(first - 1, second * 4 * size) for size, first, second in stages],
            *[table(second * 4 * size) for size, first, second in stages],
            *[table(second - 1, 4 * size) for size, first, second in stages],
            *[table(2, Z * 2 * size) for size in GROUPS] * 2,
            table(8),
            table(FEAT - 1, 8),
            dma((5,)),
            dma((groups, Z - 1)),
            dma((groups, Z - 1)),
            dma((groups, 4)),
            dma((groups, 4)),
            dma((groups, Z - 1)),
            dma((groups, Z - 1)),
            dma((FEAT - 1,)),
            dma((FEAT - 1,)),
        ],
        compiler_params=pltpu.CompilerParams(
            collective_id=0, has_side_effects=True, vmem_limit_bytes=55200 * 1024
        ),
    )(
        bin_index,
        node_ids.reshape(1, row_count),
        gradients.reshape(1, row_count),
        hessians.reshape(1, row_count),
    )
    return gains, best[0, :1]


def solution(mesh):
    in_specs = (P("feat", "rows"), P("rows"), P("rows"), P("rows"))
    out_specs = (P("rows", "feat", None), P("rows"))
    return jax.shard_map(
        per_device, mesh=mesh, in_specs=in_specs, out_specs=out_specs, check_vma=False
    )
```

```python
import functools

import jax
import jax.numpy as jnp
from jax import lax
from jax.experimental import pallas as pl
from jax.experimental.pallas import tpu as pltpu
from jax.sharding import PartitionSpec as P

BINS = 256
HALF = 128
LANES = 128
BASE = 9
TOP = 8192
X = 4
Z = 8
FEAT = 8
GROUPS = (7, 4, 3, 2)
MODES = "rzdd"
LAGS = (4, 9, 20)
BLOCK = 512
UNROLL = 16
shrinkage = 1.0
MESH = pl.DeviceIdType.MESH
f32 = jnp.float32
bf16 = jnp.bfloat16


def rows_of(row):
    return jnp.broadcast_to(row, (16, LANES)).astype(f32).astype(bf16)


def digit_rows(grad, hess):
    grad8 = jnp.broadcast_to(grad, (8, LANES))
    hess8 = jnp.broadcast_to(hess, (8, LANES))
    return jnp.concatenate([grad8, hess8], 0).astype(bf16)


def weights_of(node_ref, grad_ref, hess_ref, start, nodes_at):
    columns = []
    for tile in range(BLOCK // LANES):
        here = pl.ds(start + tile * LANES, LANES)
        node = rows_of(node_ref[0:1, here])
        grad = grad_ref[0:1, here].astype(f32)
        hess = hess_ref[0:1, here].astype(f32)
        grad_high = jnp.round(grad * (1.0 / BASE))
        hess_high = jnp.round(hess * (1.0 / BASE))
        low = digit_rows(grad - BASE * grad_high, hess - BASE * hess_high)
        high = digit_rows(grad_high, hess_high)
        none = jnp.zeros_like(low)
        masks = [node == nodes for nodes in nodes_at]
        column = [jnp.where(mask, low, none) for mask in masks]
        column += [jnp.where(mask, high, none) for mask in masks]
        columns.append(jnp.concatenate(column, 0))
    return jnp.concatenate(columns, 1)


def kernel(*refs):
    groups = len(GROUPS)
    take = iter(refs)
    some = lambda count: [next(take) for unused in range(count)]
    bins_hbm, node_hbm, grad_hbm, hess_hbm, out_ref, best_ref = some(6)
    bins_ref, node_ref, grad_ref, hess_ref, weights, total = some(6)
    partial, x_in, z_out, z_in = some(groups), some(groups), some(groups), some(groups)
    relay_in, relay_out = some(groups), some(groups)
    best_out, best_in, load_sem = some(3)
    x_send, x_recv, r_send, r_recv, z_send, z_recv, b_send, b_recv = some(8)

    feature_count, row_count = bins_ref.shape
    feat = lax.axis_index("feat")
    rows = lax.axis_index("rows")
    my_z = rows // X
    my_x = rows % X

    loads = [
        pltpu.make_async_copy(source, target, load_sem.at[number])
        for number, (source, target) in enumerate(
            [
                (node_hbm, node_ref),
                (grad_hbm, grad_ref),
                (hess_hbm, hess_ref),
                (bins_hbm.at[0:8], bins_ref.at[0:8]),
                (bins_hbm.at[8:16], bins_ref.at[8:16]),
            ]
        )
    ]
    for load in loads:
        load.start()

    def device_at(z, x):
        return ((my_z + z) % Z) * X + (my_x + x) % X

    barrier = pltpu.get_barrier_semaphore()
    for step in range(1, X):
        pl.semaphore_signal(
            barrier, inc=1, device_id=(feat, device_at(0, step)), device_id_type=MESH
        )
    for step in range(1, Z):
        pl.semaphore_signal(
            barrier, inc=1, device_id=(feat, device_at(step, 0)), device_id_type=MESH
        )
    for step in range(1, FEAT):
        pl.semaphore_signal(
            barrier, inc=1, device_id=((feat + step) % FEAT, rows), device_id_type=MESH
        )

    bin_at = lax.broadcasted_iota(jnp.int32, (HALF, LANES), 0).astype(f32).astype(bf16)
    nodes_at = [
        ((lax.broadcasted_iota(jnp.int32, (16, LANES), 0) % Z) * X + x).astype(f32).astype(bf16)
        for x in range(X)
    ]
    big = f32(1.5 * 2.0**36)

    def compute(group):
        size_here = GROUPS[group]
        base = sum(GROUPS[:group])
        totals = slice(0, size_here * HALF)

        def block(number, carry):
            start = pl.multiple_of(number * BLOCK, BLOCK)
            row_list = []
            for feature in range(size_here):
                at = base + feature
                columns = []
                for tile in range(BLOCK // LANES):
                    row = bins_ref[at : at + 1, pl.ds(start + tile * LANES, LANES)]
                    upper = row >= HALF
                    low = jnp.where(upper, row - HALF, row)
                    size = jnp.where(upper, TOP, 1)
                    low = jnp.concatenate([rows_of(low)] * (HALF // 16), 0)
                    size = jnp.concatenate([rows_of(size)] * (HALF // 16), 0)
                    columns.append(jnp.where(low <= bin_at, size, jnp.zeros_like(size)))
                row_list.append(jnp.concatenate(columns, 1))
            hot = jnp.concatenate(row_list, 0)
            if group == 0:
                weight = weights_of(node_ref, grad_ref, hess_ref, start, nodes_at)
                weights[:, pl.ds(start, BLOCK)] = weight
            else:
                weight = weights[:, pl.ds(start, BLOCK)]
            product = lax.dot_general(
                hot, weight, (((1,), (1,)), ((), ())), preferred_element_type=f32
            )
            upper_part = (product + big) - big
            total[0, totals, :] += product - upper_part
            total[1, totals, :] += upper_part
            return carry

        total[:, totals, :] = jnp.zeros((2, size_here * HALF, LANES), f32)
        lax.fori_loop(0, row_count // BLOCK, block, 0, unroll=UNROLL)
        count = 4 * size_here
        for feature in range(size_here):
            at = slice(feature * HALF, (feature + 1) * HALF)
            for half in range(2):
                turned = total[half, at, :].T
                joined = turned[: LANES // 2] + BASE * turned[LANES // 2 :]
                if half:
                    joined = joined * (1.0 / TOP)
                for x in range(X):
                    for part in range(2):
                        line = (half * 2 + part) * size_here + feature
                        from_row = x * 2 * Z + part * Z
                        if MODES[group] == "z":
                            lines = pl.ds(x * count + line, Z, stride=X * count)
                        else:
                            lines = pl.ds(x * Z * count + line, Z, stride=count)
                        partial[group][lines, :] = joined[from_row : from_row + Z]

    def lines_for(group, step):
        lines = 4 * GROUPS[group] * Z
        return pl.multiple_of(((my_x + step) % X) * lines, lines), lines

    def send(source, target, send_sem, recv_sem, device):
        return pltpu.make_async_remote_copy(
            src_ref=source,
            dst_ref=target,
            send_sem=send_sem,
            recv_sem=recv_sem,
            device_id=(feat, device),
            device_id_type=MESH,
        )

    def x_copy(group, step):
        start, lines = lines_for(group, step)
        return send(
            partial[group].at[pl.ds(start, lines)],
            x_in[group].at[step - 1],
            x_send.at[group, step - 1],
            x_recv.at[group, step - 1],
            device_at(0, step),
        )

    def far_copy(group, way):
        start, lines = lines_for(group, 2)
        half = lines // 2
        return send(
            partial[group].at[pl.ds(start + way * half, half)],
            relay_in[group].at[way],
            r_send.at[group, way],
            r_recv.at[group, way],
            device_at(0, 1 - 2 * way),
        )

    def plain_copy(group, way):
        start, lines = lines_for(group, 1 - 2 * way)
        half = lines // 2
        return send(
            partial[group].at[pl.ds(start + (1 - way) * half, half)],
            x_in[group].at[way, pl.ds((1 - way) * half, half)],
            x_send.at[group, way],
            x_recv.at[group, way],
            device_at(0, 1 - 2 * way),
        )

    def added_copy(group, way):
        half = 4 * GROUPS[group] * Z // 2
        return send(
            relay_out[group].at[way],
            x_in[group].at[way, pl.ds(way * half, half)],
            r_send.at[group, 2 + way],
            r_recv.at[group, 2 + way],
            device_at(0, 1 - 2 * way),
        )

    def z_copy(group, step):
        lines = 4 * GROUPS[group]
        source = pl.multiple_of(((my_z + step) % Z) * lines, lines)
        return pltpu.make_async_remote_copy(
            src_ref=z_out[group].at[pl.ds(source, lines)],
            dst_ref=z_in[group].at[step - 1],
            send_sem=z_send.at[group, step - 1],
            recv_sem=z_recv.at[group, step - 1],
            device_id=(feat, device_at(step, 0)),
            device_id_type=MESH,
        )

    def z_first_copy(group, step):
        lines = 4 * GROUPS[group] * X
        start = pl.multiple_of(((my_z + step) % Z) * lines, lines)
        return send(
            partial[group].at[pl.ds(start, lines)],
            x_in[group].at[step - 1],
            x_send.at[group, step - 1],
            x_recv.at[group, step - 1],
            device_at(step, 0),
        )

    def x_last_copy(group, step):
        lines = 4 * GROUPS[group]
        start = pl.multiple_of(((my_x + step) % X) * lines, lines)
        return send(
            z_out[group].at[pl.ds(start, lines)],
            z_in[group].at[step - 1],
            z_send.at[group, step - 1],
            z_recv.at[group, step - 1],
            device_at(0, step),
        )

    def best_copy(step):
        return pltpu.make_async_remote_copy(
            src_ref=best_out,
            dst_ref=best_in.at[step - 1],
            send_sem=b_send.at[step - 1],
            recv_sem=b_recv.at[step - 1],
            device_id=((feat + step) % FEAT, rows),
            device_id_type=MESH,
        )

    def start_x(group):
        if MODES[group] == "r":
            for way in range(2):
                far_copy(group, way).start()
            for way in range(2):
                plain_copy(group, way).start()
        elif MODES[group] == "z":
            for step in (4, 3, 5, 2, 6, 1, 7):
                z_first_copy(group, step).start()
        else:
            for step in (2, 1, 3):
                x_copy(group, step).start()

    def relay(group):
        for way in range(2):
            far_copy(group, way).wait_recv()
            start, lines = lines_for(group, 1 - 2 * way)
            half = lines // 2
            mine = partial[group][pl.ds(start + way * half, half), :]
            relay_out[group][way] = relay_in[group][way] + mine
            added_copy(group, way).start()

    def z_to_x(group):
        lines = 4 * GROUPS[group] * X
        summed = partial[group][pl.ds(pl.multiple_of(my_z * lines, lines), lines), :]
        for step in range(1, Z):
            z_first_copy(group, step).wait_recv()
            summed = summed + x_in[group][step - 1]
        z_out[group][...] = summed
        for step in (2, 1, 3):
            x_last_copy(group, step).start()

    def x_to_z(group):
        if MODES[group] == "z":
            return z_to_x(group)
        start, lines = lines_for(group, 0)
        summed = partial[group][pl.ds(start, lines), :]
        if MODES[group] == "r":
            for way in range(2):
                plain_copy(group, way).wait_recv()
                added_copy(group, way).wait_recv()
                summed = summed + x_in[group][way]
        else:
            for step in range(1, X):
                x_copy(group, step).wait_recv()
                summed = summed + x_in[group][step - 1]
        z_out[group][...] = summed
        for step in (4, 3, 5, 2, 6, 1, 7):
            z_copy(group, step).start()

    def gains_at(group, summed):
        size = GROUPS[group]
        base = sum(GROUPS[:group])
        first = summed[: 2 * size]
        second = summed[2 * size :] + first[:, HALF - 1 :]
        whole = second[:, HALF - 1 :]
        whole_grad, whole_hess = whole[:size], whole[size:]
        unsplit = whole_grad * whole_grad / (whole_hess + shrinkage)
        for half, left in enumerate((first, second)):
            right = whole - left
            left_grad, left_hess = left[:size], left[size:]
            right_grad, right_hess = right[:size], right[size:]
            out_ref[0, base : base + size, half * HALF : (half + 1) * HALF] = 0.5 * (
                left_grad * left_grad / (left_hess + shrinkage)
                + right_grad * right_grad / (right_hess + shrinkage)
                - unsplit
            )

    def finish(group):
        if MODES[group] == "z":
            lines = 4 * GROUPS[group]
            summed = z_out[group][pl.ds(pl.multiple_of(my_x * lines, lines), lines), :]
            for step in range(1, X):
                x_last_copy(group, step).wait_recv()
                summed = summed + z_in[group][step - 1]
            return gains_at(group, summed)
        for step in range(1, Z):
            z_copy(group, step).wait_recv()
        lines = 4 * GROUPS[group]
        summed = z_out[group][pl.ds(pl.multiple_of(my_z * lines, lines), lines), :]
        for step in range(1, Z):
            summed = summed + z_in[group][step - 1]
        gains_at(group, summed)

    for number in range(4):
        loads[number].wait()
    events = []
    done = 0
    for group in range(groups):
        done += GROUPS[group]
        relayed = MODES[group] != "d"
        if MODES[group] == "r":
            events.append((done + LAGS[0], 0, group, relay))
        events.append((done + LAGS[relayed], 1, group, x_to_z))
        events.append((done + LAGS[relayed] + LAGS[2] - LAGS[1], 2, group, finish))
    events.sort(key=lambda event: event[:3])
    done = 0
    for group in range(groups):
        compute(group)
        done += GROUPS[group]
        if group == 0:
            loads[4].wait()
            pl.semaphore_wait(barrier, X - 1 + Z - 1 + FEAT - 1)
        start_x(group)
        while events and (events[0][0] <= done or group == groups - 1):
            unused_time, unused_stage, which, action = events.pop(0)
            action(which)
    gains = out_ref[0]
    top = jnp.max(jnp.max(gains, axis=1, keepdims=True), axis=0, keepdims=True)
    best_out[...] = jnp.broadcast_to(top, best_out.shape)
    for step in (4, 5, 3, 2, 6, 7, 1):
        best_copy(step).start()
    for group in range(groups):
        if MODES[group] == "r":
            for way in range(2):
                far_copy(group, way).wait_send()
                plain_copy(group, way).wait_send()
                added_copy(group, way).wait_send()
        elif MODES[group] == "d":
            for step in range(1, X):
                x_copy(group, step).wait_send()
        if MODES[group] == "z":
            for step in range(1, Z):
                z_first_copy(group, step).wait_send()
            for step in range(1, X):
                x_last_copy(group, step).wait_send()
        else:
            for step in range(1, Z):
                z_copy(group, step).wait_send()
    best = best_out[...]
    for step in range(1, FEAT):
        best_copy(step).wait_recv()
        best = jnp.maximum(best, best_in[step - 1])
    best_ref[...] = jnp.broadcast_to(best, best_ref.shape)
    for step in range(1, FEAT):
        best_copy(step).wait_send()


def per_device(bin_index, node_ids, gradients, hessians):
    feature_count, row_count = bin_index.shape
    groups = len(GROUPS)
    vmem = pl.BlockSpec(memory_space=pltpu.VMEM)
    hbm = pl.BlockSpec(memory_space=pltpu.HBM)
    dma = pltpu.SemaphoreType.DMA
    stages = [(size, *((Z, X) if mode == "z" else (X, Z))) for size, mode in zip(GROUPS, MODES)]
    table = lambda *shape: pltpu.VMEM((*shape, LANES), f32)
    gains, best = pl.pallas_call(
        kernel,
        out_shape=(
            jax.ShapeDtypeStruct((1, feature_count, BINS), f32),
            jax.ShapeDtypeStruct((8, LANES), f32),
        ),
        in_specs=[hbm] * 4,
        out_specs=(vmem, vmem),
        scratch_shapes=[
            pltpu.VMEM((feature_count, row_count), jnp.int32),
            *[pltpu.VMEM((1, row_count), jnp.int32)] * 3,
            pltpu.VMEM((LANES, row_count), bf16),
            table(2, max(GROUPS) * HALF),
            *[table(X * Z * 4 * size) for size in GROUPS],
            *[table(first - 1, second * 4 * size) for size, first, second in stages],
            *[table(second * 4 * size) for size, first, second in stages],
            *[table(second - 1, 4 * size) for size, first, second in stages],
            *[table(2, Z * 2 * size) for size in GROUPS] * 2,
            table(1),
            table(FEAT - 1, 1),
            dma((5,)),
            dma((groups, Z - 1)),
            dma((groups, Z - 1)),
            dma((groups, 4)),
            dma((groups, 4)),
            dma((groups, Z - 1)),
            dma((groups, Z - 1)),
            dma((FEAT - 1,)),
            dma((FEAT - 1,)),
        ],
        compiler_params=pltpu.CompilerParams(
            collective_id=0, has_side_effects=True, vmem_limit_bytes=55200 * 1024
        ),
    )(
        bin_index,
        node_ids.reshape(1, row_count),
        gradients.reshape(1, row_count),
        hessians.reshape(1, row_count),
    )
    return gains, best[0, :1]


def solution(mesh):
    in_specs = (P("feat", "rows"), P("rows"), P("rows"), P("rows"))
    out_specs = (P("rows", "feat", None), P("rows"))
    return jax.shard_map(
        per_device, mesh=mesh, in_specs=in_specs, out_specs=out_specs, check_vma=False
    )
```
